32 devices in a mesh: dp: 4 (over y, x), mp: 8 (over z, core).
Axes of the slice: x: 2, y: 2, z: 4, core: 2. Of those that a mesh axis runs over, the one named last changes fastest.
Arguments:
- stored: float32 [16384, 18432], P(('dp', 'mp')), may hold values from -0.046875 to 0.046875
- row_map: int32 [16384], replicated, may hold values from 0 to 16383, as said below
- probe: bfloat16 [16384, 1024], P('dp'), may hold values from -6 to 6
- lane: bfloat16 [128, 1024], replicated, may hold values from -6 to 6
Outputs:
- shards: bfloat16 [144, 128, 16384], P('mp', None, 'dp')
- slab_checks: float32 [144, 32, 1024], P('mp', 'dp')
- head_sums: float32 [144, 1024], P('mp')
The draws below stay inside these ranges and needn't reach their ends.
Inputs may be any that keep to these rules, and one draw needn't show every extreme that they name: row_map is a permutation of 0..16383 with row_map[i] // 4096 == (i % 512) // 128 for every stored row i.
All inputs are finite; a program needn't handle non-finite values.
Results may differ from the reference program's by a relative error of at most 0.0029.
Values may be sent and summed in bfloat16 or wider, within the bound.
A program may use at most 128 MiB of HBM per device.

```python
import jax
import jax.numpy as jnp
from jax import lax

D = 16384
Q_HEADS = 128
KV_HEADS = 8
HD = 128
PROBES = 1024
SLABS = 8
QKV = 18432
ROWS_DEV = 512
SUB_ROWS = 128
GROUP_ROWS = 4096
DP_GROUPS = 4
SLAB = 512
SLOTS = 18
N_DP = 4
N_MP = 8


def draw_row_map(key, part):
    stored_index = jnp.arange(D, dtype=jnp.int32)
    target_group = stored_index % ROWS_DEV // SUB_ROWS
    rank_inside = stored_index // ROWS_DEV * SUB_ROWS + stored_index % SUB_ROWS
    group_keys = jax.random.split(jax.random.fold_in(key, 17), DP_GROUPS)
    shuffled = jax.vmap(lambda one_key: jax.random.permutation(one_key, GROUP_ROWS))(group_keys).astype(jnp.int32)
    return (target_group * GROUP_ROWS + shuffled[target_group, rank_inside]).astype(jnp.int32)


def levels(rng, dims, pieces, least, high):
    def one(axis_at, blocks):
        heights = jax.random.uniform(jax.random.fold_in(jax.random.fold_in(rng, 6), axis_at), (blocks,), jnp.float32, least / len(pieces), high / len(pieces))
        return jnp.repeat(jnp.exp(heights), dims[axis_at] // blocks).reshape((-1,) + (1,) * (len(dims) - axis_at - 1))

    factor_of = one(*pieces[0])
    for cut in pieces[1:]:
        factor_of = factor_of * one(*cut)
    return factor_of


def scatter_about(stream_key, dims, deviation, reach, cuts=(), kind=jnp.bfloat16):
    entries = deviation * jax.random.normal(stream_key, dims, jnp.float32)
    if cuts:
        entries = entries * levels(stream_key, dims, cuts, -0.22, 0.18)
    return jnp.clip(entries, -reach, reach).astype(kind)


def setup_inputs(seed: int = 0) -> dict:
    arg_keys = jax.random.split(jax.random.key(seed), 5)
    return {
        "stored": scatter_about(arg_keys[0], (D, QKV), D ** -0.5, 0.046875, ((0, 32),), jnp.float32),
        "row_map": draw_row_map(jax.random.fold_in(arg_keys[4], 71), 0),
        "probe": scatter_about(arg_keys[2], (D, PROBES), 1.0, 6.0, ((0, 4),)),
        "lane": scatter_about(arg_keys[3], (HD, PROBES), 1.0, 6.0),
    }


def reference(stored, row_map, probe, lane):
    weights = jnp.zeros((D, QKV), jnp.bfloat16).at[row_map].set(stored.astype(jnp.bfloat16))
    head_cols = weights.reshape(D, Q_HEADS + 2 * KV_HEADS, HD)
    kv_index = (jnp.arange(N_MP, dtype=jnp.int32) * KV_HEADS) // N_MP
    query_cols = head_cols[:, :Q_HEADS].reshape(D, N_MP, Q_HEADS // N_MP, HD)
    key_cols = head_cols[:, Q_HEADS + kv_index][:, :, None]
    value_cols = head_cols[:, Q_HEADS + KV_HEADS + kv_index][:, :, None]
    slotted = jnp.concatenate([query_cols, key_cols, value_cols], axis=2)
    shards = jnp.transpose(slotted, (1, 2, 3, 0)).reshape(N_MP * SLOTS, HD, D)
    lane_wide = lane.astype(jnp.float32)

    def one_slab(slab_start):
        slab_block = lax.dynamic_slice_in_dim(shards, slab_start, SLAB, 2).astype(jnp.float32)
        probe_rows = lax.dynamic_slice_in_dim(probe, slab_start, SLAB, 0).astype(jnp.float32)
        projected = jnp.einsum("jer,rp->jep", slab_block, probe_rows, precision=lax.Precision.HIGHEST)
        return jnp.sum(projected * lane_wide[None], axis=1)

    slab_starts = jnp.arange(N_DP * SLABS, dtype=jnp.int32) * SLAB
    stacked = lax.map(one_slab, slab_starts)
    slab_checks = jnp.transpose(stacked, (1, 0, 2))
    head_sums = jnp.mean(slab_checks, axis=1)
    return shards, slab_checks, head_sums
```

```python
import functools

import jax
import jax.numpy as jnp
from jax import lax
from jax.experimental import pallas as pl
from jax.experimental.pallas import tpu as pltpu
from jax.sharding import PartitionSpec as P

Q_HEADS = 128
KV_HEADS = 8
HD = 128
SLABS = 8
PAIR = 2
AHEAD = 3
MESH = pl.DeviceIdType.MESH


def kernel(
    n_dp, n_mp, stored, local_row, probe, lane,
    shards, checks, heads, narrow, landing,
    onehot, wide, cast, arrived, turned, placed, slab_sums, sums,
    load_sem, local_sem, send_sem, recv_sem, out_sem, sum_send, sum_recv,
):
    my_dp = lax.axis_index("dp")
    my_mp = lax.axis_index("mp")
    n_dev = n_dp * n_mp
    me = my_dp * n_mp + my_mp
    rows_dev = stored.shape[0]
    sub = rows_dev // n_dp
    group_rows = probe.shape[0]
    slab_rows = group_rows // SLABS
    per_device = Q_HEADS // n_mp
    slots = per_device + 2
    share = n_mp // KV_HEADS
    chunks = slots // PAIR
    width = PAIR * HD

    barrier = pltpu.get_barrier_semaphore()

    def peer(k):
        return lax.rem(my_dp + k // n_mp, n_dp), lax.rem(my_mp + lax.rem(k, n_mp), n_mp)

    @pl.loop(1, n_dev)
    def _(k):
        pl.semaphore_signal(barrier, inc=1, device_id=peer(k), device_id_type=MESH)

    def load(step):
        copies = []
        for m in range(n_mp):
            if isinstance(step, int) and step == 0:
                for pos, head in enumerate((Q_HEADS + m // share, Q_HEADS + KV_HEADS + m // share)):
                    copies.append((stored.at[:, pl.ds(head * HD, HD)], wide.at[m, :, pl.ds(pos * HD, HD)]))
            else:
                first = pl.multiple_of((m * per_device + (step - 1) * PAIR) * HD, HD)
                copies.append((stored.at[:, pl.ds(first, width)], wide.at[m]))
        for src, dst in copies:
            pltpu.make_async_copy(src, dst, load_sem).start()
        pltpu.make_async_copy(wide, wide, load_sem).wait()

    def issue(step):
        load(step)

        @pl.loop(0, n_dp)
        def _(d):
            for m in range(n_mp):
                cast[d * n_mp + m] = wide[m, pl.ds(pl.multiple_of(d * sub, sub), sub), :].astype(jnp.bfloat16)

        to_narrow = pltpu.make_async_copy(cast, narrow.at[step], local_sem.at[0])
        own = pltpu.make_async_copy(cast.at[me], landing.at[step, me], local_sem.at[1])
        to_narrow.start()
        own.start()
        to_narrow.wait()
        own.wait()

        @pl.loop(1, n_dev)
        def _(k):
            dp, mp = peer(k)
            pltpu.make_async_remote_copy(
                src_ref=narrow.at[step, dp * n_mp + mp],
                dst_ref=landing.at[step, me],
                send_sem=send_sem.at[step],
                recv_sem=recv_sem.at[step],
                device_id=(dp, mp),
                device_id_type=MESH,
            ).start()

    pl.semaphore_wait(barrier, n_dev - 1)
    ahead = min(AHEAD, chunks)
    for step in range(ahead):
        issue(step)

    @pl.loop(0, SLABS)
    def _(i):
        rows = pl.ds(pl.multiple_of(i * slab_rows, slab_rows), slab_rows)
        target = local_row[rows, :]

        @pl.loop(0, SLABS)
        def _(j):
            first = pl.multiple_of(j * slab_rows, slab_rows)
            column = lax.broadcasted_iota(jnp.int32, (slab_rows, slab_rows), 1) + first
            onehot[rows, pl.ds(first, slab_rows)] = jnp.where(column == target, 1.0, 0.0).astype(jnp.bfloat16)

    group = max(1, HD // sub)
    span = group * sub

    def all_of(step):
        part = landing.at[step, pl.ds(0, n_dev - 1)]
        return pltpu.make_async_copy(part, part, recv_sem.at[step])

    def out_copy(first_slot):
        return pltpu.make_async_copy(placed, shards.at[pl.ds(first_slot, PAIR)], out_sem)

    @pl.loop(0, chunks)
    def _(step):
        first_slot = lax.rem(step * PAIR + per_device, slots)

        @pl.when(step + ahead < chunks)
        def _():
            issue(step + ahead)

        all_of(step).wait()
        fetch = pltpu.make_async_copy(landing.at[step], arrived, local_sem.at[0])
        fetch.start()
        fetch.wait()

        @pl.loop(0, n_dev // group)
        def _(b):
            rows = arrived[pl.ds(b * group, group)].astype(jnp.float32).reshape(span, width)
            turned[:, pl.ds(pl.multiple_of(b * span, span), span)] = rows.T.astype(jnp.bfloat16)

        @pl.when(step > 0)
        def _():
            out_copy(0).wait()

        @pl.loop(0, SLABS)
        def _(s):
            rows = pl.ds(pl.multiple_of(s * slab_rows, slab_rows), slab_rows)
            block = jnp.dot(turned[...], onehot[:, rows], preferred_element_type=jnp.float32).astype(jnp.bfloat16)
            placed[:, :, rows] = block.reshape(PAIR, HD, slab_rows)
            projected = jnp.dot(block, probe[rows, :], preferred_element_type=jnp.float32)
            weighted = projected.reshape(PAIR, HD, -1) * lane[...].astype(jnp.float32)[None]
            slab_sums[s] = jnp.sum(weighted, axis=1)

        out_copy(first_slot).start()
        for s in range(SLABS):
            for pos in range(PAIR):
                checks[first_slot + pos, s : s + 1, :] = slab_sums[s, pos : pos + 1, :]

    sums[my_dp] = jnp.sum(checks[...], axis=1)
    out_copy(0).wait()

    @pl.loop(1, n_dp)
    def _(k):
        pltpu.make_async_remote_copy(
            src_ref=sums.at[my_dp],
            dst_ref=sums.at[my_dp],
            send_sem=sum_send,
            recv_sem=sum_recv,
            device_id=(lax.rem(my_dp + k, n_dp), my_mp),
            device_id_type=MESH,
        ).start()

    others = sums.at[pl.ds(0, n_dp - 1)]
    pltpu.make_async_copy(others, others, sum_recv).wait()
    pltpu.make_async_copy(others, others, sum_send).wait()
    total = sums[0]
    for d in range(1, n_dp):
        total = total + sums[d]
    heads[...] = total / (n_dp * SLABS)

    @pl.loop(0, chunks)
    def _(step):
        part = narrow.at[step, pl.ds(0, n_dev - 1)]
        pltpu.make_async_copy(part, part, send_sem.at[step]).wait()


def body(stored, row_map, probe, lane):
    n_dp = lax.axis_size("dp")
    n_mp = lax.axis_size("mp")
    n_dev = n_dp * n_mp
    rows_dev, cols = stored.shape
    sub = rows_dev // n_dp
    group_rows, probes = probe.shape
    slots = Q_HEADS // n_mp + 2
    chunks = slots // PAIR
    width = PAIR * HD
    my_dp = lax.axis_index("dp")
    local_row = lax.dynamic_index_in_dim(row_map.reshape(n_dev, n_dp, sub), my_dp, 1, False)
    local_row = local_row.reshape(group_rows, 1) - my_dp * group_rows
    vmem = pl.BlockSpec(memory_space=pltpu.VMEM)
    hbm = pl.BlockSpec(memory_space=pl.ANY)
    moved = jax.ShapeDtypeStruct((chunks, n_dev, sub, width), jnp.bfloat16)
    shards, checks, heads, _, _ = pl.pallas_call(
        functools.partial(kernel, n_dp, n_mp),
        out_shape=(
            jax.ShapeDtypeStruct((slots, HD, group_rows), jnp.bfloat16),
            jax.ShapeDtypeStruct((slots, SLABS, probes), jnp.float32),
            jax.ShapeDtypeStruct((slots, probes), jnp.float32),
            moved,
            moved,
        ),
        in_specs=[hbm, vmem, vmem, vmem],
        out_specs=(hbm, vmem, vmem, hbm, hbm),
        scratch_shapes=[
            pltpu.VMEM((group_rows, group_rows), jnp.bfloat16),
            pltpu.VMEM((n_mp, rows_dev, width), jnp.float32),
            pltpu.VMEM((n_dev, sub, width), jnp.bfloat16),
            pltpu.VMEM((n_dev, sub, width), jnp.bfloat16),
            pltpu.VMEM((width, group_rows), jnp.bfloat16),
            pltpu.VMEM((PAIR, HD, group_rows), jnp.bfloat16),
            pltpu.VMEM((SLABS, PAIR, probes), jnp.float32),
            pltpu.VMEM((n_dp, slots, probes), jnp.float32),
            pltpu.SemaphoreType.DMA,
            pltpu.SemaphoreType.DMA((2,)),
            pltpu.SemaphoreType.DMA((chunks,)),
            pltpu.SemaphoreType.DMA((chunks,)),
            pltpu.SemaphoreType.DMA,
            pltpu.SemaphoreType.DMA,
            pltpu.SemaphoreType.DMA,
        ],
        compiler_params=pltpu.CompilerParams(
            collective_id=0, has_side_effects=True, vmem_limit_bytes=66_000_000
        ),
    )(stored, local_row, probe, lane)
    return shards, checks, heads


def solution(mesh):
    return jax.shard_map(
        body,
        mesh=mesh,
        in_specs=(P(("dp", "mp"), None), P(), P("dp", None), P()),
        out_specs=(P("mp", None, "dp"), P("mp", "dp", None), P("mp", None)),
        check_vma=False,
    )
```
